32 devices in a mesh: grp: 2 (over x), gx: 8 (over z, y), gz: 2 (over core).
Axes of the slice: x: 2, y: 2, z: 4, core: 2. Of those that a mesh axis runs over, the one named last changes fastest.
Arguments:
- electric: float32 [512, 8192], P(('grp', 'gx'), 'gz'), parts along dimension 0, may hold values from -6 to 6
- magnetic_x: float32 [512, 8192], P(('grp', 'gx'), 'gz'), parts along dimension 0, may hold values from -6 to 6
- magnetic_z: float32 [512, 8192], P(('grp', 'gx'), 'gz'), parts along dimension 0, may hold values from -6 to 6
- index_map: int32 [4, 64, 8192], P(None, None, 'gz'), may hold values from 0 to 3
- period_seq: int32 [10], P('grp'), parts along dimension 0, may hold values from 0 to 3
- eps_table: float32 [4], replicated, may hold values from 1 to 12.25
- shifts: int32 [8], P('grp'), parts along dimension 0, may hold values from 0 to 4, as said below
Outputs:
- electric_out: float32 [512, 8192], P(('grp', 'gx'), 'gz'), parts along dimension 0
- magnetic_x_out: float32 [512, 8192], P(('grp', 'gx'), 'gz'), parts along dimension 0
- magnetic_z_out: float32 [512, 8192], P(('grp', 'gx'), 'gz'), parts along dimension 0
The draws below stay inside these ranges and needn't reach their ends.
There are 2 independent parts, one for each index of `grp`. The reference program is written for one: setup_inputs(seed, part) draws one part's arguments, and reference() takes and returns one part's arrays. A program takes and returns all parts, laid end to end along the dimension named above; an argument that names none is the same for every part. Nothing has to cross between parts.
Inputs may be any that keep to these rules, and one draw needn't show every extreme that they name: `shifts`: every entry is at most 4, and some entry equals 4.
All inputs are finite; a program needn't handle non-finite values.
Results may differ from the reference program's by a relative error of at most 0.00016.
Values sent between devices are 32-bit elements; how exact they have to be, the bound alone decides.
No kernel may reach another device: no remote copies, remote signals or barrier semaphores. Data moves between devices by JAX's collectives and lax.ppermute only.
A program may use at most 64 MiB of HBM per device.

```python
import math
import jax
import jax.numpy as jnp
from jax import lax

ITERS = 4
SMAX = 4
PER = 64
TYPES = 4
LEVELS = 4
NX = 256
NZ = 8192
NP = 5


def draw_shifts(key, part):
    values = jax.random.randint(key, (ITERS,), 0, SMAX + 1, dtype=jnp.int32)
    where_most = jax.random.randint(jax.random.fold_in(key, 7), (), 0, ITERS, dtype=jnp.int32)
    return values.at[where_most].set(SMAX)


def plant(result, key, smallest, top_value):
    dims = result.shape
    spot = [jax.random.randint(jax.random.fold_in(key, axis), (), 0, dims[axis]) for axis in range(len(dims))]
    result = result.at[tuple(spot)].set(smallest)
    longest = dims.index(max(dims))
    spot[longest] = (spot[longest] + 1) % dims[longest]
    return result.at[tuple(spot)].set(top_value)


def block_levels(rng, shape, shards, low, top_value):
    gain = 1.0
    for axis_at, parts in shards:
        heights = jax.random.uniform(jax.random.fold_in(jax.random.fold_in(rng, 6), axis_at), (parts,), jnp.float32, low / len(shards), top_value / len(shards))
        gain = gain * jnp.repeat(jnp.exp(heights), shape[axis_at] // parts).reshape((-1,) + (1,) * (len(shape) - 1 - axis_at))
    return gain


def noise(rng, extent, deviation, limit, cuts=(), kind=jnp.bfloat16):
    result = deviation * jax.random.normal(rng, extent, jnp.float32)
    if cuts:
        result = result * block_levels(rng, extent, cuts, -0.22, 0.18)
    return jnp.clip(result, -limit, limit).astype(kind)


def setup_inputs(seed: int = 0, part: int = 0) -> dict:
    key_list = jax.random.split(jax.random.key(seed), 8)
    part_keys = jax.random.split(jax.random.fold_in(key_list[7], part), 8)
    electric = noise(part_keys[0], (NX, NZ), 1.0, 6.0, ((0, 8), (1, 2)), jnp.float32)
    magnetic_x = noise(part_keys[1], (NX, NZ), 1.0, 6.0, ((0, 8), (1, 2)), jnp.float32)
    magnetic_z = noise(part_keys[2], (NX, NZ), 1.0, 6.0, ((0, 8), (1, 2)), jnp.float32)
    index_map = plant(jax.random.randint(key_list[3], (TYPES, PER, NZ), 0, LEVELS), jax.random.fold_in(key_list[3], 1), 0, LEVELS - 1).astype(jnp.int32)
    period_seq = plant(jax.random.randint(part_keys[4], (NP,), 0, TYPES), jax.random.fold_in(part_keys[4], 1), 0, TYPES - 1).astype(jnp.int32)
    eps_table = jnp.clip(jnp.exp(jax.random.uniform(key_list[5], (LEVELS,), jnp.float32, math.log(1.0), math.log(12.25))), 1.0, 12.25)
    shifts = draw_shifts(jax.random.fold_in(jax.random.fold_in(key_list[7], part), 71), part)
    return dict(electric=electric, magnetic_x=magnetic_x, magnetic_z=magnetic_z, index_map=index_map, period_seq=period_seq, eps_table=eps_table, shifts=shifts)


def reference(electric, magnetic_x, magnetic_z, index_map, period_seq, eps_table, shifts):
    inverse = 1.0 / eps_table
    total_x, total_z = electric.shape
    offset = jnp.int32(0)
    tail = jnp.zeros((SMAX, total_z), electric.dtype)
    fields = [electric, magnetic_x, magnetic_z]
    for step in range(ITERS):
        moved = shifts[step].astype(jnp.int32)
        offset = offset + moved
        fields = [lax.dynamic_slice_in_dim(jnp.concatenate([item, tail], axis=0), moved, total_x, 0) for item in fields]
        columns = jnp.arange(total_x, dtype=jnp.int32) + offset
        design = period_seq[columns // PER]
        layers = jnp.arange(total_z, dtype=jnp.int32)
        levels = index_map[design[:, None], (columns % PER)[:, None], layers[None, :]]
        coeff = inverse[levels]
        field_e, field_hx, field_hz = fields
        zero_col = jnp.zeros((total_x, 1), field_e.dtype)
        zero_row = jnp.zeros((1, total_z), field_e.dtype)
        upper = jnp.concatenate([field_e[:, 1:], zero_col], axis=1)
        field_hx = field_hx + 0.6 * (upper - field_e)
        ahead = jnp.concatenate([field_e[1:], zero_row], axis=0)
        field_hz = field_hz - 0.6 * (ahead - field_e)
        lower = jnp.concatenate([zero_col, field_hx[:, :-1]], axis=1)
        behind = jnp.concatenate([zero_row, field_hz[:-1]], axis=0)
        field_e = field_e + 0.6 * coeff * ((field_hx - lower) - (field_hz - behind))
        fields = [field_e, field_hx, field_hz]
    return fields[0], fields[1], fields[2]
```

```python
import functools

import jax
import jax.numpy as jnp
from jax import lax
from jax.experimental import pallas as pl
from jax.experimental.pallas import tpu as pltpu
from jax.sharding import PartitionSpec as P

ITERS = 4
SMAX = 4
LANES = 128
TILE = 8
OUTER = 16

courant = 0.6

VMEM = pltpu.VMEM
ANY = pl.ANY


def up(value, unit):
    return -(-value // unit) * unit


def spec(space):
    return pl.BlockSpec(memory_space=space)


def sides(gz):
    return gz == 0


def pack_kernel(plan, part, e, hx, hz, out, buf, sem):
    low = lax.axis_index("gz") == 0
    count = plan.count[part]
    start = jnp.where(low, plan.start_low[part], plan.start_high[part]) * LANES
    start = pl.multiple_of(start, LANES)
    rows = buf.shape[1]
    copies = [
        pltpu.make_async_copy(
            field.at[pl.ds(0, rows), pl.ds(start, count * LANES)], buf.at[i], sem.at[i]
        )
        for i, field in enumerate((e, hx, hz))
    ]
    for copy in copies:
        copy.start()
    for copy in copies:
        copy.wait()
    for strip in range(count):
        for i in range(3):
            for q in range(rows // TILE):
                at = strip * plan.sent + plan.place[i] + q * TILE
                out[pl.ds(at, TILE), :] = buf[i, pl.ds(q * TILE, TILE), pl.ds(strip * LANES, LANES)]


def material_of(levels, inverse):
    result = jnp.zeros(levels.shape, jnp.float32)
    for level, value in enumerate(inverse):
        result = jnp.where(levels == level, value, result)
    return result


def inverse_table(eps):
    return [courant * (1.0 / jnp.full((TILE, LANES), eps[i], jnp.float32)) for i in range(eps.shape[0])]


def map_rows(plan, period_seq, index_map, group, first, width):
    span = index_map.shape[1]
    cell = lax.axis_index("gx") * plan.rows + group * TILE
    period = jnp.minimum(cell // span, period_seq.shape[0] - 1)
    phase = pl.multiple_of(cell % span, TILE)
    return index_map.at[period_seq[period], pl.ds(phase, TILE), pl.ds(first, width)]


def edge_kernel(plan, period_seq, eps, e, hx, hz, index_map, out, levels, sem):
    low = lax.axis_index("gz") == 0
    first = pl.multiple_of(jnp.where(low, plan.strips - 1, 0) * LANES, LANES)
    rows = plan.rows
    copies = [
        pltpu.make_async_copy(
            field.at[:, pl.ds(first, LANES)], out.at[pl.ds(i * rows, rows), :], sem.at[i]
        )
        for i, field in enumerate((e, hx, hz))
    ]
    for group in range(plan.reach // TILE):
        copies.append(
            pltpu.make_async_copy(
                map_rows(plan, period_seq, index_map, group, first, LANES),
                levels.at[pl.ds(group * TILE, TILE), :],
                sem.at[3 + group],
            )
        )
    for copy in copies:
        copy.start()
    for copy in copies:
        copy.wait()
    inverse = inverse_table(eps)
    for group in range(plan.reach // TILE):
        at = pl.ds(group * TILE, TILE)
        out[pl.ds(3 * rows + group * TILE, TILE), :] = material_of(levels[at, :], inverse)


def prepare_kernel(plan, period_seq, eps, e, hx, hz, index_map, e_out, hx_out, hz_out, coeff, levels, sem):
    width = plan.strips * LANES
    fields = [
        pltpu.make_async_copy(src, dst, sem.at[i])
        for i, (src, dst) in enumerate(((e, e_out), (hx, hx_out), (hz, hz_out)))
    ]
    groups = plan.reach // TILE
    maps = [
        pltpu.make_async_copy(
            map_rows(plan, period_seq, index_map, group, 0, width),
            levels.at[pl.ds(group * TILE, TILE), :],
            sem.at[3 + group],
        )
        for group in range(groups)
    ]
    for copy in maps + fields:
        copy.start()
    inverse = inverse_table(eps)
    for group in range(groups):
        maps[group].wait()
        at = pl.ds(group * TILE, TILE)

        def strip_of(strip, _, at=at):
            lanes = pl.ds(pl.multiple_of(strip * LANES, LANES), LANES)
            coeff[at, lanes] = material_of(levels[at, lanes], inverse)
            return 0

        lax.fori_loop(0, plan.strips, strip_of, 0, unroll=8)
    for copy in fields:
        copy.wait()


def update_kernel(plan, part, shifts, *refs):
    fields, coeff, halo, halo_lead, leads = refs[0:3], refs[3], refs[4], refs[5], refs[6 : 7 + part]
    refs = refs[7 + part :]
    if part:
        refs = refs[3:]
    outs, work, work_coeff, stage, sem = refs[0:3], refs[3:6], refs[6], refs[7], refs[8]
    low = lax.axis_index("gz") == 0
    rows, reach, strips = plan.rows, plan.reach, plan.strips
    lead_rows = reach - rows
    local = plan.local[part]

    def own(strip, to):
        lanes = pl.ds(pl.multiple_of(strip * LANES, LANES), LANES)
        for i in range(3):
            work[i][to, pl.ds(0, rows), :] = fields[i][:, lanes]
        work_coeff[to] = coeff[:, lanes]

    def lead(source, at, to):
        for i in range(3):
            for q in range(lead_rows // TILE):
                work[i][to, pl.ds(rows + q * TILE, TILE), :] = source[pl.ds(at + plan.place[i] + q * TILE, TILE), :]

    for i in range(3):
        work[i][local] = jnp.zeros((reach, LANES), jnp.float32)
    inner, outer = plan.count
    if part == 0:
        shift = jnp.where(low, 0, 1)
        first = jnp.where(low, outer, 0)

        def gather(k, _):
            own(first + k, shift + k)
            lead(leads[0], k * plan.sent, shift + k)
            return 0

        lax.fori_loop(0, inner, gather, 0)
        side = jnp.where(low, inner, 0)
        for i in range(3):
            work[i][side, pl.ds(0, rows), :] = halo[pl.ds(i * rows, rows), :]
        work_coeff[side] = halo[pl.ds(3 * rows, reach), :]
        lead(halo_lead, 0, side)
        done, kept = 1, inner - 1
        column = jnp.where(low, outer + 1, 0)
    else:
        shift = jnp.where(low, 0, 2)
        first = jnp.where(low, 0, inner)

        def gather(k, _):
            own(first + k, shift + k)
            lead(leads[1], k * plan.sent, shift + k)
            return 0

        lax.fori_loop(0, outer, gather, 0)
        for k in range(2):
            strip = jnp.where(low, outer + k, inner - 2 + k)
            to = jnp.where(low, outer + k, k)
            own(strip, to)
            lead(leads[0], jnp.where(low, k, inner - 2 + k) * plan.sent, to)
        done, kept = jnp.where(low, 0, 1), outer + 1
        column = jnp.where(low, 0, inner - 1)

    row = lax.broadcasted_iota(jnp.int32, (reach, LANES), 0)
    lane = lax.broadcasted_iota(jnp.int32, (reach, LANES), 1)
    start = lax.axis_index("gx") * rows
    total = lax.axis_size("gx") * rows
    offset = jnp.int32(0)
    for step in range(ITERS):
        offset = offset + shifts[step]
        above = row >= offset - start
        below = row < offset + total - start

        def strip_step(strip, carry):
            turned, hx_before = carry
            field_e = work[0][strip]
            turned_next = pltpu.roll(work[0][strip + 1], LANES - 1, 1)
            upper = jnp.where(lane == LANES - 1, turned_next, turned)
            field_hx = work[1][strip] + courant * (upper - field_e)
            ahead = pltpu.roll(field_e, reach - 1, 0)
            field_hz = work[2][strip] - courant * (ahead - field_e)
            field_hz = jnp.where(above, field_hz, 0.0)
            hx_turned = pltpu.roll(field_hx, 1, 1)
            lower = jnp.where(lane == 0, hx_before, hx_turned)
            behind = pltpu.roll(field_hz, 1, 0)
            moved = field_e + work_coeff[strip] * ((field_hx - lower) - (field_hz - behind))
            work[0][strip] = jnp.where(below, moved, 0.0)
            work[1][strip] = field_hx
            work[2][strip] = field_hz
            return turned_next, hx_turned

        none = jnp.zeros((reach, LANES), jnp.float32)
        lax.fori_loop(0, local, strip_step, (pltpu.roll(work[0][0], LANES - 1, 1), none))

    def finish(k, _):
        lanes = pl.ds(pl.multiple_of(k * LANES, LANES), LANES)
        for i in range(3):
            for q in range(rows // TILE):
                stage[i, pl.ds(q * TILE, TILE), lanes] = work[i][done + k, pl.ds(offset + q * TILE, TILE), :]
        return 0

    lax.fori_loop(0, kept, finish, 0)
    column = pl.multiple_of(column * LANES, LANES)
    copies = [
        pltpu.make_async_copy(stage.at[i], outs[i].at[:, pl.ds(column, kept * LANES)], sem.at[i])
        for i in range(3)
    ]
    for copy in copies:
        copy.start()
    for copy in copies:
        copy.wait()


class Plan:
    def __init__(self, rows, cols, moved):
        self.rows = rows
        self.strips = cols // LANES
        self.reach = up(rows + ITERS * SMAX + ITERS, TILE)
        outer = OUTER
        inner = self.strips - outer
        self.count = (inner, outer)
        self.start_low = (outer, 0)
        self.start_high = (0, inner)
        self.local = (inner + 1, outer + 2)
        lead_e, lead_h = moved + ITERS, moved + ITERS - 1
        self.place = (0, lead_e, lead_e + lead_h)
        self.sent = lead_e + 2 * lead_h
        self.head = up(lead_e, TILE)

        self.window = up(self.place[2] + self.reach - rows, TILE)

    def buffer(self, part):
        return up((self.count[part] - 1) * self.sent + self.window, TILE)


def call(kernel, name, outs, ins, out_spaces, scratch, aliases=None, flops=1):
    return pl.pallas_call(
        kernel,
        name=name,
        out_shape=outs,
        in_specs=[spec(space) for space in ins],
        out_specs=[spec(space) for space in out_spaces],
        scratch_shapes=scratch,
        input_output_aliases=aliases or {},
        cost_estimate=pl.CostEstimate(flops=flops, bytes_accessed=flops, transcendentals=0),
        compiler_params=pltpu.CompilerParams(vmem_limit_bytes=16 << 20),
    )


def f32(*shape):
    return jax.ShapeDtypeStruct(shape, jnp.float32)


def advance(moved, electric, magnetic_x, magnetic_z, index_map, period_seq, eps_table, shifts):
    rows, cols = electric.shape
    plan = Plan(rows, cols, moved)
    strips, reach = plan.strips, plan.reach
    fields = (electric, magnetic_x, magnetic_z)
    count_x = lax.axis_size("gx")
    back = [(i + 1, i) for i in range(count_x - 1)]
    swap = [(0, 1), (1, 0)]
    leads = []
    for part in range(2):
        packed = call(
            functools.partial(pack_kernel, plan, part),
            f"pack{part}",
            [f32(plan.buffer(part), LANES)],
            [ANY] * 3,
            [VMEM],
            [VMEM((3, plan.head, plan.count[part] * LANES), jnp.float32), pltpu.SemaphoreType.DMA((3,))],
        )(*fields)[0]
        leads.append(lax.ppermute(packed, "gx", back))
    groups = reach // TILE
    edge = call(
        functools.partial(edge_kernel, plan),
        "edge",
        [f32(3 * rows + reach, LANES)],
        [pltpu.SMEM] * 2 + [ANY] * 4,
        [VMEM],
        [VMEM((reach, LANES), jnp.int32), pltpu.SemaphoreType.DMA((3 + groups,))],
    )(period_seq, eps_table, *fields, index_map)[0]
    halo = lax.ppermute(edge, "gz", swap)
    *held, coeff = call(
        functools.partial(prepare_kernel, plan),
        "prepare",
        [f32(rows, cols)] * 3 + [f32(reach, cols)],
        [pltpu.SMEM] * 2 + [ANY] * 4,
        [VMEM] * 4,
        [VMEM((reach, cols), jnp.int32), pltpu.SemaphoreType.DMA((3 + groups,))],
    )(period_seq, eps_table, *fields, index_map)
    at = jnp.where(lax.axis_index("gz") == 0, plan.count[0] - 1, 0) * plan.sent
    halo_lead = lax.ppermute(
        lax.dynamic_slice_in_dim(leads[0], at, plan.window, 0), "gz", swap
    )
    outs = ()
    for part in range(2):
        kept = (plan.count[0] - 1, plan.count[1] + 1)[part]
        work = [VMEM((plan.local[part] + 1, reach, LANES), jnp.float32)] * 4
        outs = call(
            functools.partial(update_kernel, plan, part),
            f"update{part}",
            [f32(rows, cols)] * 3,
            [pltpu.SMEM] + [VMEM] * (7 + part) + [ANY] * len(outs),
            [ANY] * 3,
            work + [VMEM((3, rows, kept * LANES), jnp.float32), pltpu.SemaphoreType.DMA((3,))],
            {8 + part + i: i for i in range(len(outs))},
        )(shifts, *held, coeff, halo, halo_lead, *leads[: 1 + part], *outs)
    return tuple(outs)


def body(electric, magnetic_x, magnetic_z, index_map, period_seq, eps_table, shifts):
    return advance(ITERS * SMAX, electric, magnetic_x, magnetic_z, index_map, period_seq, eps_table, shifts)


def solution(mesh):
    assert mesh.shape["gz"] == 2
    placed = (
        P(("grp", "gx"), "gz"),
        P(("grp", "gx"), "gz"),
        P(("grp", "gx"), "gz"),
        P(None, None, "gz"),
        P("grp"),
        P(),
        P("grp"),
    )
    return jax.shard_map(
        body,
        mesh=mesh,
        in_specs=placed,
        out_specs=(P(("grp", "gx"), "gz"), P(("grp", "gx"), "gz"), P(("grp", "gx"), "gz")),
        check_vma=False,
    )
```

```python
import functools

import jax
import jax.numpy as jnp
from jax import lax
from jax.experimental import pallas as pl
from jax.experimental.pallas import tpu as pltpu
from jax.sharding import PartitionSpec as P

ITERS = 4
SMAX = 4
LANES = 128
TILE = 8
OUTER = 16
AHEAD = 4
BOUNDS = tuple(range(SMAX + 2, ITERS * SMAX + 1, 2))

courant = 0.6

VMEM = pltpu.VMEM
HBM = pltpu.HBM


def up(value, unit):
    return -(-value // unit) * unit


def spec(space):
    return pl.BlockSpec(memory_space=space)


def pack_kernel(
    plan, bounds, period_seq, eps, shifts, e, hx, hz, index_map, inner_out, outer_out, which_out,
    buf, levels, coeff, *scratch,
):
    work, sem = scratch[:-1], scratch[-1]
    low = lax.axis_index("gz") == 0
    strips, head = plan.strips, buf.shape[1]
    groups = head // TILE
    copies = [pltpu.make_async_copy(field.at[pl.ds(0, head), :], buf.at[i], sem.at[i]) for i, field in enumerate((e, hx, hz))]
    for group in range(groups):
        copies.append(
            pltpu.make_async_copy(
                map_rows(plan, period_seq, index_map, group, 0, strips * LANES),
                levels.at[pl.ds(group * TILE, TILE), :],
                sem.at[3 + group],
            )
        )
    for copy in copies:
        copy.start()
    total = way(shifts)
    which = jnp.int32(0)
    bound = jnp.int32(bounds[0])
    for now, after in zip(bounds[:-1], bounds[1:]):
        which = which + (total > now).astype(jnp.int32)
        bound = bound + jnp.where(total > now, after - now, 0)
    which_out[0] = which
    base = jnp.maximum(total - ITERS, 0)
    inverse = inverse_table(eps)
    for copy in copies:
        copy.wait()

    fields, source = work[0:3], work[3:6]
    for strip in range(strips):
        lanes = pl.ds(strip * LANES, LANES)
        for i in range(3):
            source[i][strip] = buf[i, :, lanes]
        source_levels = work[6]
        source_levels[strip] = levels[:, lanes]
    sets = [fields] + [work[7 + 4 * k : 11 + 4 * k] for k in range(ITERS - 1)]

    def read(step, i, strip):
        if step == 0:
            return source[i][strip, pl.ds(base, TILE), :]
        return sets[step][i][strip]

    def factor(step, strip):
        if step == 0:
            coeff[strip] = material_of(work[6][strip, pl.ds(base, TILE), :], inverse)
        return coeff[strip]

    def write(step, strip, *values):
        for ref, value in zip(sets[step + 1], values):
            ref[strip] = value

    march(ITERS - 1, strips, TILE, read, factor, write)

    sent = 3 * bound + ITERS
    place = (0, bound + 1, 2 * bound + 1, 3 * bound + 1)

    def put(out, at, strip):
        for i in range(3):
            for q in range(groups):
                out[pl.ds(at + place[i] + q * TILE, TILE), :] = source[i][strip, pl.ds(q * TILE, TILE), :]
        for step in range(1, ITERS):
            out[pl.ds(at + place[3] + step - 1, 1), :] = sets[step][0][strip, pl.ds(ITERS, 1), :]

    inner, outer = plan.count
    for k in range(inner):
        put(inner_out, k * sent, jnp.where(low, outer + k, inner - 1 - k))
    for i in range(3):
        side = jnp.where(low, strips - 1, 0)
        inner_out[pl.ds(inner * sent + i * TILE, TILE), :] = source[i][side, pl.ds(bound, TILE), :]
    for k in range(outer):
        put(outer_out, k * sent, jnp.where(low, k, inner + k))


def way(shifts):
    total = shifts[0]
    for step in range(1, ITERS):
        total = total + shifts[step]
    return total


def march(steps, strips, used, read, factor, write, mask=None):
    lane = lax.broadcasted_iota(jnp.int32, (used, LANES), 1)
    last_lane, first_lane = lane == LANES - 1, lane == 0
    none = jnp.zeros((used, LANES), jnp.float32)
    for step in range(steps):
        above, below = mask(step) if mask else (None, None)
        values, left, right, hx_right = {}, {strips: none}, {-1: none}, {-1: none}
        for strip in range(-AHEAD, strips):
            coming = strip + AHEAD
            if coming < strips:
                values[coming] = read(step, 0, coming)
                left[coming] = pltpu.roll(values[coming], LANES - 1, 1)
                right[coming] = pltpu.roll(values[coming], 1, 1)
                if step == 0:
                    hx_right[coming] = pltpu.roll(read(step, 1, coming), 1, 1)
            if strip < 0:
                continue
            field_e = values.pop(strip)
            upper = jnp.where(last_lane, left[strip + 1], left[strip])
            under = jnp.where(first_lane, right[strip - 1], right[strip])
            if step == 0:
                lower = jnp.where(first_lane, hx_right[strip - 1], hx_right[strip])
            else:
                lower = read(step, 3, strip)
            field_hx = read(step, 1, strip) + courant * (upper - field_e)
            lower = lower + courant * (field_e - under)
            if strip == 0:
                lower = jnp.where(first_lane, 0.0, lower)
            ahead = pltpu.roll(field_e, used - 1, 0)
            field_hz = read(step, 2, strip) - courant * (ahead - field_e)
            if above is not None:
                field_hz = jnp.where(above, field_hz, 0.0)
            behind = pltpu.roll(field_hz, 1, 0)
            moved = field_e + factor(step, strip) * ((field_hx - lower) - (field_hz - behind))
            if below is not None:
                moved = jnp.where(below, moved, 0.0)
            write(step, strip, moved, field_hx, field_hz, lower)


def material_of(levels, inverse):
    result = jnp.zeros(levels.shape, jnp.float32)
    for level, value in enumerate(inverse):
        result = jnp.where(levels == level, value, result)
    return result


def inverse_table(eps):
    return [courant * (1.0 / jnp.full((TILE, LANES), eps[i], jnp.float32)) for i in range(eps.shape[0])]


def map_rows(plan, period_seq, index_map, group, first, width):
    span = index_map.shape[1]
    cell = lax.axis_index("gx") * plan.rows + group * TILE
    period = jnp.minimum(cell // span, period_seq.shape[0] - 1)
    phase = pl.multiple_of(cell % span, TILE)
    return index_map.at[period_seq[period], pl.ds(phase, TILE), pl.ds(first, width)]


def prepare_kernel(
    plan, period_seq, eps, e, hx, hz, index_map, edge, e_out, hx_out, hz_out, coeff,
    levels, edge_sem, field_sem, sem,
):
    low = lax.axis_index("gz") == 0
    first = pl.multiple_of(jnp.where(low, plan.strips - 1, 0) * LANES, LANES)
    rows, strips = plan.rows, plan.strips
    groups = plan.reach // TILE
    fields = (e, hx, hz)
    edges = [
        pltpu.make_async_copy(
            field.at[:, pl.ds(first, LANES)], edge.at[pl.ds(i * rows, rows), :], edge_sem.at[i]
        )
        for i, field in enumerate(fields)
    ]
    maps = [
        pltpu.make_async_copy(
            map_rows(plan, period_seq, index_map, group, 0, strips * LANES),
            levels.at[pl.ds(group * TILE, TILE), :],
            sem.at[group],
        )
        for group in range(groups)
    ]
    for copy in edges + maps:
        copy.start()

    def field_copy(i, strip):
        return pltpu.make_async_copy(
            fields[i].at[:, pl.ds(pl.multiple_of(strip * LANES, LANES), LANES)],
            (e_out, hx_out, hz_out)[i].at[strip, pl.ds(0, rows), :],
            field_sem.at[i, strip],
        )

    def start_strip(strip, _):
        for i in range(3):
            field_copy(i, strip).start()
        return 0

    lax.fori_loop(0, strips, start_strip, 0)
    inverse = inverse_table(eps)
    for copy in maps:
        copy.wait()

    def strip_of(strip, _):
        lanes = pl.ds(pl.multiple_of(strip * LANES, LANES), LANES)
        for group in range(groups):
            at = pl.ds(group * TILE, TILE)
            coeff[strip, at, :] = material_of(levels[at, lanes], inverse)
        return 0

    lax.fori_loop(0, strips, strip_of, 0, unroll=2)
    for group in range(groups):
        at = pl.ds(group * TILE, TILE)
        edge[pl.ds(3 * rows + group * TILE, TILE), :] = material_of(levels[at, pl.ds(first, LANES)], inverse)
    for copy in edges:
        copy.wait()

    def wait_strip(strip, _):
        for i in range(3):
            field_copy(i, strip).wait()
        return 0

    lax.fori_loop(0, strips, wait_strip, 0)


def update_kernel(plan, part, shifts, *refs):
    fields, coeff, halo, halo_lead, leads = refs[0:3], refs[3], refs[4], refs[5], refs[6 : 7 + part]
    refs = refs[7 + part :]
    if part:
        refs = refs[3:]
    outs, source, source_coeff, source_behind = refs[0:3], refs[3:6], refs[6], refs[7]
    work, work_coeff, stage, sem = refs[8:16], refs[16], refs[17], refs[18]
    low = lax.axis_index("gz") == 0
    rows, reach, used = plan.rows, plan.reach, plan.used
    lead_rows = reach - rows
    local = plan.local[part]

    def own(strip, to):
        for i in range(3):
            source[i][to, pl.ds(0, rows), :] = fields[i][strip, pl.ds(0, rows), :]
        source_coeff[to] = coeff[strip]

    def lead(sent, at, to):
        for i in range(3):
            for q in range(lead_rows // TILE):
                source[i][to, pl.ds(rows + q * TILE, TILE), :] = sent[pl.ds(at + plan.place[i] + q * TILE, TILE), :]
        source_behind[to] = sent[pl.ds(at + plan.place[3], TILE), :]

    def lead_side(sent, at, to):
        for i in range(3):
            source[i][to, pl.ds(rows + plan.moved, TILE), :] = sent[pl.ds(at + i * TILE, TILE), :]

    inner, outer = plan.count
    if part == 0:
        for k in range(inner):
            strip = jnp.where(low, outer + k, inner - 1 - k)
            to = jnp.where(low, k, inner - k)
            own(strip, to)
            lead(leads[0], k * plan.sent, to)
        lead_side(leads[0], inner * plan.sent, jnp.where(low, inner - 1, 1))
        side = jnp.where(low, inner, 0)
        for i in range(3):
            source[i][side, pl.ds(0, rows), :] = halo[pl.ds(i * rows, rows), :]
        source_coeff[side] = halo[pl.ds(3 * rows, reach), :]
        lead(halo_lead, plan.side, side)
        lead_side(halo_lead, plan.side + plan.sent, side)
        done, kept = 1, inner - 1
        column = jnp.where(low, outer + 1, 0)
    else:
        for k in range(outer):
            to = jnp.where(low, k, k + 2)
            own(jnp.where(low, k, inner + k), to)
            lead(leads[1], k * plan.sent, to)
        for k in range(2):
            to = jnp.where(low, outer + k, 1 - k)
            own(jnp.where(low, outer + k, inner - 1 - k), to)
            lead(leads[0], k * plan.sent, to)
        done, kept = jnp.where(low, 0, 1), outer + 1
        column = jnp.where(low, 0, inner - 1)

    row = lax.broadcasted_iota(jnp.int32, (used, LANES), 0)
    total = lax.axis_size("gx") * rows
    base = jnp.maximum(way(shifts) - ITERS, 0)
    start = lax.axis_index("gx") * rows + base
    sets = (work[0:4], work[4:8])
    lane = lax.broadcasted_iota(jnp.int32, (1, LANES), 1)
    half = LANES // 2
    known = {}
    if part == 0:
        known[0] = (0, LANES), (LANES, LANES)
        known[1] = (0, LANES), (half, LANES)
        known[inner - 1] = (0, half), (0, LANES)
        known[inner] = (0, 0), (0, LANES)

    def mask(step):
        offset = shifts[0]
        for earlier in range(step):
            offset = offset + shifts[earlier + 1]
        return row >= offset - start, row < offset + total - start

    def read(step, i, strip):
        if step == 0:
            return source[i][strip, pl.ds(base, used), :]
        return sets[step % 2][i][strip]

    def factor(step, strip):
        if step == 0:
            work_coeff[strip] = source_coeff[strip, pl.ds(base, used), :]
        return work_coeff[strip]

    def write(step, strip, *values):
        later = sets[(step + 1) % 2]
        for ref, value in zip(later, values):
            ref[strip] = value
        if step + 1 < ITERS:
            behind = source_behind[strip, pl.ds(step, 1), :]
            at = pl.ds(rows + ITERS, 1)
            if strip in known:
                lows, highs = known[strip]
                inside = (lane >= jnp.where(low, lows[0], highs[0])) & (lane < jnp.where(low, lows[1], highs[1]))
                behind = jnp.where(inside, behind, values[0][rows + ITERS : rows + ITERS + 1])
            later[0][strip, at, :] = behind

    march(ITERS, local, used, read, factor, write, mask)
    for k in range(kept):
        lanes = pl.ds(k * LANES, LANES)
        for i, ref in enumerate(sets[ITERS % 2][0:3]):
            stage[i, :, lanes] = ref[done + k, pl.ds(ITERS, rows), :]
    column = pl.multiple_of(column * LANES, LANES)
    copies = [
        pltpu.make_async_copy(stage.at[i], outs[i].at[:, pl.ds(column, kept * LANES)], sem.at[i])
        for i in range(3)
    ]
    for copy in copies:
        copy.start()
    for copy in copies:
        copy.wait()


class Plan:
    def __init__(self, rows, cols, moved):
        assert rows % TILE == 0 and cols % LANES == 0
        self.rows = rows
        self.strips = cols // LANES
        self.reach = up(rows + ITERS * SMAX + ITERS, TILE)
        self.used = up(rows + 2 * ITERS, TILE)
        self.head = self.reach - rows
        assert rows >= self.head and self.used <= self.reach
        self.count = (self.strips - OUTER, OUTER)
        self.local = (self.count[0] + 1, OUTER + 2)
        self.moved = moved
        self.place = (0, moved + 1, 2 * moved + 1, 3 * moved + 1)
        self.sent = 3 * moved + ITERS
        first = (self.count[0] - 1) * self.sent
        self.cut = first // TILE * TILE
        self.side = first - self.cut

    def buffer(self, part):
        behind = max(self.place[2] + self.head, self.place[3] + TILE)
        end = (self.count[part] - 1) * self.sent + behind
        return up(max(end, self.count[part] * self.sent + 3 * TILE), TILE)


def call(kernel, name, outs, ins, out_spaces, scratch, aliases=None, flops=1 << 20):
    return pl.pallas_call(
        kernel,
        name=name,
        out_shape=outs,
        in_specs=[spec(space) for space in ins],
        out_specs=[spec(space) for space in out_spaces],
        scratch_shapes=scratch,
        input_output_aliases=aliases or {},
        cost_estimate=pl.CostEstimate(flops=flops, bytes_accessed=flops, transcendentals=0),
        compiler_params=pltpu.CompilerParams(vmem_limit_bytes=16 << 20),
    )


def f32(*shape):
    return VMEM(shape, jnp.float32)


def advance(moved, inner_sent, outer_sent, electric, magnetic_x, magnetic_z, index_map, period_seq, eps_table, shifts):
    rows, cols = electric.shape
    plan = Plan(rows, cols, moved)
    strips, reach = plan.strips, plan.reach
    fields = (electric, magnetic_x, magnetic_z)
    count_x = lax.axis_size("gx")
    back = [(i + 1, i) for i in range(count_x - 1)]
    swap = [(0, 1), (1, 0)]
    leads = [
        lax.ppermute(lax.slice_in_dim(packed, 0, plan.buffer(part), axis=0), "gx", back)
        for part, packed in enumerate((inner_sent, outer_sent))
    ]
    groups = reach // TILE
    edge, *held, coeff = call(
        functools.partial(prepare_kernel, plan),
        "prepare",
        [f32(3 * rows + reach, LANES)] + [f32(strips, reach, LANES)] * 4,
        [pltpu.SMEM] * 2 + [HBM] * 4,
        [VMEM] * 5,
        [
            VMEM((reach, cols), jnp.int32),
            pltpu.SemaphoreType.DMA((3,)),
            pltpu.SemaphoreType.DMA((3, strips)),
            pltpu.SemaphoreType.DMA((groups,)),
        ],
    )(period_seq, eps_table, *fields, index_map)
    halo = lax.ppermute(edge, "gz", swap)
    halo_lead = lax.ppermute(lax.slice_in_dim(leads[0], plan.cut, None, axis=0), "gz", swap)
    outs = ()
    for part in range(2):
        kept = (plan.count[0] - 1, plan.count[1] + 1)[part]
        local = plan.local[part]
        work = [VMEM((local, reach, LANES), jnp.float32)] * 4 + [VMEM((local, TILE, LANES), jnp.float32)]
        work += [VMEM((local, plan.used, LANES), jnp.float32)] * 9
        outs = call(
            functools.partial(update_kernel, plan, part),
            f"update{part}",
            [HBM((rows, cols), jnp.float32)] * 3,
            [pltpu.SMEM] + [VMEM] * (7 + part) + [HBM] * len(outs),
            [HBM] * 3,
            work + [VMEM((3, rows, kept * LANES), jnp.float32), pltpu.SemaphoreType.DMA((3,))],
            {8 + part + i: i for i in range(len(outs))},
        )(shifts, *held, coeff, halo, halo_lead, *leads[: 1 + part], *outs)
    return tuple(outs)


def body(electric, magnetic_x, magnetic_z, index_map, period_seq, eps_table, shifts):
    rows, cols = electric.shape
    electric, magnetic_x, magnetic_z, index_map = (
        pltpu.with_memory_space_constraint(item, HBM) for item in (electric, magnetic_x, magnetic_z, index_map)
    )
    rest = (electric, magnetic_x, magnetic_z, index_map, period_seq, eps_table, shifts)
    plan = Plan(rows, cols, BOUNDS[-1])
    strips, head = plan.strips, plan.head
    inner_sent, outer_sent, which = call(
        functools.partial(pack_kernel, plan, BOUNDS),
        "pack",
        [f32(plan.buffer(0), LANES), f32(plan.buffer(1), LANES), pltpu.SMEM((1,), jnp.int32)],
        [pltpu.SMEM] * 3 + [HBM] * 4,
        [VMEM, VMEM, pltpu.SMEM],
        [
            VMEM((3, head, cols), jnp.float32),
            VMEM((head, cols), jnp.int32),
            VMEM((strips, TILE, LANES), jnp.float32),
        ]
        + [VMEM((strips, TILE, LANES), jnp.float32)] * 3
        + [VMEM((strips, head, LANES), jnp.float32)] * 3
        + [VMEM((strips, head, LANES), jnp.int32)]
        + [VMEM((strips, TILE, LANES), jnp.float32)] * (4 * (ITERS - 1))
        + [pltpu.SemaphoreType.DMA((3 + head // TILE,))],
    )(period_seq, eps_table, shifts, electric, magnetic_x, magnetic_z, index_map)
    return lax.switch(which[0], [functools.partial(advance, bound) for bound in BOUNDS], inner_sent, outer_sent, *rest)


def solution(mesh):
    assert mesh.shape["gz"] == 2
    placed = (
        P(("grp", "gx"), "gz"),
        P(("grp", "gx"), "gz"),
        P(("grp", "gx"), "gz"),
        P(None, None, "gz"),
        P("grp"),
        P(),
        P("grp"),
    )
    return jax.shard_map(
        body,
        mesh=mesh,
        in_specs=placed,
        out_specs=(P(("grp", "gx"), "gz"), P(("grp", "gx"), "gz"), P(("grp", "gx"), "gz")),
        check_vma=False,
    )
```

```python
import functools

import jax
import jax.numpy as jnp
from jax import lax
from jax.experimental import pallas as pl
from jax.experimental.pallas import tpu as pltpu
from jax.sharding import PartitionSpec as P

ITERS = 4
SMAX = 4
LANES = 128
TILE = 8
OUTER = 12
AHEAD = 4
GROUPS = 3
BOUNDS = (*range(2 * SMAX, ITERS * SMAX - 1), ITERS * SMAX)

courant = 0.6

VMEM = pltpu.VMEM
HBM = pltpu.HBM


def up(value, unit):
    return -(-value // unit) * unit


def spec(space):
    return pl.BlockSpec(memory_space=space)


def pack_kernel(
    plan, bounds, *refs
):
    tables, (e, hx, hz, index_map, inner_out, outer_out, which_out, moves_out) = refs[0:3], refs[3:11]
    (period_seq, eps, shifts), (buf, levels, coeff), work, sem = refs[11:14], refs[14:17], refs[17:-1], refs[-1]
    low = lax.axis_index("gz") == 0
    strips, head = plan.strips, buf.shape[1]
    groups = head // TILE
    scalars = [
        pltpu.make_async_copy(src, dst, sem.at[i]) for i, (src, dst) in enumerate(zip(tables, (period_seq, eps, shifts)))
    ]
    copies = [
        pltpu.make_async_copy(
            field.at[pl.ds(q * TILE, TILE), :], buf.at[i, pl.ds(q * TILE, TILE), :], sem.at[3 + groups * i + q]
        )
        for i, field in enumerate((e, hx, hz))
        for q in range(groups)
    ]
    for copy in scalars + copies:
        copy.start()
    for copy in scalars:
        copy.wait()
    maps = [
        pltpu.make_async_copy(
            map_rows(plan, period_seq, index_map, group, 0, strips * LANES),
            levels.at[pl.ds(group * TILE, TILE), :],
            sem.at[3 + groups * 3 + group],
        )
        for group in range(groups)
    ]
    for copy in maps:
        copy.start()
    total = way(shifts)
    which = jnp.int32(0)
    bound = jnp.int32(bounds[0])
    for now, after in zip(bounds[:-1], bounds[1:]):
        which = which + (total > now).astype(jnp.int32)
        bound = bound + jnp.where(total > now, after - now, 0)
    for step in range(ITERS):
        moves_out[step] = shifts[step]
    which_out[0] = which
    base = jnp.maximum(total - ITERS, 0)
    inverse = inverse_table(eps)
    for copy in copies:
        copy.wait()
    fields, source = work[0:3], work[3:6]
    for strip in range(strips):
        for i in range(3):
            source[i][strip] = buf[i, :, pl.ds(strip * LANES, LANES)]

    sent = 3 * bound + ITERS
    place = (0, bound + 1, 2 * bound + 1, 3 * bound + 1)
    inner, outer = plan.count

    def each(put):
        for k in range(inner):
            put(inner_out, k * sent, jnp.where(low, outer + k, inner - 1 - k))
        for k in range(outer):
            put(outer_out, k * sent, jnp.where(low, k, inner + k))

    def put_fields(out, at, strip):
        for i in range(3):
            for q in range(groups):
                out[pl.ds(at + place[i] + q * TILE, TILE), :] = source[i][strip, pl.ds(q * TILE, TILE), :]

    each(put_fields)
    for i in range(3):
        side = jnp.where(low, strips - 1, 0)
        inner_out[pl.ds(inner * sent + i * TILE, TILE), :] = source[i][side, pl.ds(bound, TILE), :]

    for copy in maps:
        copy.wait()
    for strip in range(strips):
        work[6][strip] = levels[:, pl.ds(strip * LANES, LANES)]
    sets = [fields] + [work[7 + 4 * k : 11 + 4 * k] for k in range(ITERS - 1)]

    def read(step, i, strip):
        if step == 0:
            return source[i][strip, pl.ds(base, TILE), :]
        return sets[step][i][strip]

    def factor(step, strip):
        if step == 0:
            coeff[strip] = material_of(work[6][strip, pl.ds(base, TILE), :], inverse)
        return coeff[strip]

    def write(step, strip, *values):
        for ref, value in zip(sets[step + 1], values):
            ref[strip] = value

    march(ITERS - 1, strips, TILE, read, factor, write)

    def put_behind(out, at, strip):
        for step in range(1, ITERS):
            out[pl.ds(at + place[3] + step - 1, 1), :] = sets[step][0][strip, pl.ds(ITERS, 1), :]

    each(put_behind)


def way(shifts):
    total = shifts[0]
    for step in range(1, ITERS):
        total = total + shifts[step]
    return total


def march(steps, strips, used, read, factor, write, mask=None):
    lane = lax.broadcasted_iota(jnp.int32, (used, LANES), 1)
    last_lane, first_lane = lane == LANES - 1, lane == 0
    none = jnp.zeros((used, LANES), jnp.float32)
    for step in range(steps):
        above, below = mask(step) if mask else (None, None)
        values, left, right, hx_right = {}, {strips: none}, {-1: none}, {-1: none}
        for strip in range(-AHEAD, strips):
            coming = strip + AHEAD
            if coming < strips:
                values[coming] = read(step, 0, coming)
                left[coming] = pltpu.roll(values[coming], LANES - 1, 1)
                right[coming] = pltpu.roll(values[coming], 1, 1)
                if step == 0:
                    hx_right[coming] = pltpu.roll(read(step, 1, coming), 1, 1)
            if strip < 0:
                continue
            field_e = values.pop(strip)
            upper = jnp.where(last_lane, left[strip + 1], left[strip])
            under = jnp.where(first_lane, right[strip - 1], right[strip])
            if step == 0:
                lower = jnp.where(first_lane, hx_right[strip - 1], hx_right[strip])
            else:
                lower = read(step, 3, strip)
            field_hx = read(step, 1, strip) + courant * (upper - field_e)
            lower = lower + courant * (field_e - under)
            if strip == 0:
                lower = jnp.where(first_lane, 0.0, lower)
            ahead = pltpu.roll(field_e, used - 1, 0)
            field_hz = read(step, 2, strip) - courant * (ahead - field_e)
            if above is not None:
                field_hz = jnp.where(above, field_hz, 0.0)
            behind = pltpu.roll(field_hz, 1, 0)
            moved = field_e + factor(step, strip) * ((field_hx - lower) - (field_hz - behind))
            if below is not None:
                moved = jnp.where(below, moved, 0.0)
            write(step, strip, moved, field_hx, field_hz, lower)


def material_of(levels, inverse):
    result = jnp.zeros(levels.shape, jnp.float32)
    for level, value in enumerate(inverse):
        result = jnp.where(levels == level, value, result)
    return result


def inverse_table(eps):
    return [courant * (1.0 / jnp.full((TILE, LANES), eps[i], jnp.float32)) for i in range(eps.shape[0])]


def map_rows(plan, period_seq, index_map, group, first, width):
    span = index_map.shape[1]
    cell = lax.axis_index("gx") * plan.rows + group * TILE
    period = jnp.minimum(cell // span, period_seq.shape[0] - 1)
    phase = pl.multiple_of(cell % span, TILE)
    return index_map.at[period_seq[period], pl.ds(phase, TILE), pl.ds(first, width)]


def prepare_kernel(
    plan, period_seq, eps, e, hx, hz, index_map, edge, e_out, hx_out, hz_out, coeff,
    levels, edge_sem, field_sem, sem,
):
    low = lax.axis_index("gz") == 0
    first = pl.multiple_of(jnp.where(low, plan.strips - 1, 0) * LANES, LANES)
    rows, strips = plan.rows, plan.strips
    groups = plan.reach // TILE
    fields = (e, hx, hz)
    edges = [
        pltpu.make_async_copy(
            field.at[:, pl.ds(first, LANES)], edge.at[pl.ds(i * rows, rows), :], edge_sem.at[i]
        )
        for i, field in enumerate(fields)
    ]
    maps = [
        pltpu.make_async_copy(
            map_rows(plan, period_seq, index_map, group, 0, strips * LANES),
            levels.at[pl.ds(group * TILE, TILE), :],
            sem.at[group],
        )
        for group in range(groups)
    ]
    for copy in edges + maps:
        copy.start()

    def field_copy(i, strip):
        return pltpu.make_async_copy(
            fields[i].at[:, pl.ds(pl.multiple_of(strip * LANES, LANES), LANES)],
            (e_out, hx_out, hz_out)[i].at[strip, pl.ds(0, rows), :],
            field_sem.at[i, strip],
        )

    def start_strip(strip, _):
        for i in range(3):
            field_copy(i, strip).start()
        return 0

    lax.fori_loop(0, strips, start_strip, 0)
    inverse = inverse_table(eps)
    for copy in maps:
        copy.wait()

    def strip_of(strip, _):
        lanes = pl.ds(pl.multiple_of(strip * LANES, LANES), LANES)
        for group in range(groups):
            at = pl.ds(group * TILE, TILE)
            coeff[strip, at, :] = material_of(levels[at, lanes], inverse)
        return 0

    lax.fori_loop(0, strips, strip_of, 0, unroll=2)
    for group in range(groups):
        at = pl.ds(group * TILE, TILE)
        edge[pl.ds(3 * rows + group * TILE, TILE), :] = material_of(levels[at, pl.ds(first, LANES)], inverse)
    for copy in edges:
        copy.wait()

    def wait_strip(strip, _):
        for i in range(3):
            field_copy(i, strip).wait()
        return 0

    lax.fori_loop(0, strips, wait_strip, 0)


def update_kernel(plan, part, shifts, *refs):
    fields, coeff, halo, halo_lead, leads = refs[0:3], refs[3], refs[4], refs[5], refs[6 : 7 + part]
    refs = refs[7 + part :]
    if part:
        refs = refs[3:]
    outs, source, source_coeff, source_behind = refs[0:3], refs[3:6], refs[6], refs[7]
    work, work_coeff, stage, sem = refs[8:16], refs[16], refs[17], refs[18]
    low = lax.axis_index("gz") == 0
    rows, reach, used = plan.rows, plan.reach, plan.used
    lead_rows = reach - rows
    local = plan.local[part]

    def own(strip, to):
        for i in range(3):
            source[i][to, pl.ds(0, rows), :] = fields[i][strip, pl.ds(0, rows), :]
        source_coeff[to] = coeff[strip]

    def lead(sent, at, to):
        for i in range(3):
            for q in range(lead_rows // TILE):
                source[i][to, pl.ds(rows + q * TILE, TILE), :] = sent[pl.ds(at + plan.place[i] + q * TILE, TILE), :]
        source_behind[to] = sent[pl.ds(at + plan.place[3], TILE), :]

    def lead_side(sent, at, to):
        for i in range(3):
            source[i][to, pl.ds(rows + plan.moved, TILE), :] = sent[pl.ds(at + i * TILE, TILE), :]

    inner, outer = plan.count
    if part == 0:
        for k in range(inner):
            strip = jnp.where(low, outer + k, inner - 1 - k)
            to = jnp.where(low, k, inner - k)
            own(strip, to)
            lead(leads[0], k * plan.sent, to)
        lead_side(leads[0], inner * plan.sent, jnp.where(low, inner - 1, 1))
        side = jnp.where(low, inner, 0)
        for i in range(3):
            source[i][side, pl.ds(0, rows), :] = halo[pl.ds(i * rows, rows), :]
        source_coeff[side] = halo[pl.ds(3 * rows, reach), :]
        lead(halo_lead, plan.side, side)
        lead_side(halo_lead, plan.side + plan.sent, side)
        done, kept = 1, inner - 1
        column = jnp.where(low, outer + 1, 0)
    else:
        for k in range(outer):
            to = jnp.where(low, k, k + 2)
            own(jnp.where(low, k, inner + k), to)
            lead(leads[1], k * plan.sent, to)
        for k in range(2):
            to = jnp.where(low, outer + k, 1 - k)
            own(jnp.where(low, outer + k, inner - 1 - k), to)
            lead(leads[0], k * plan.sent, to)
        done, kept = jnp.where(low, 0, 1), outer + 1
        column = jnp.where(low, 0, inner - 1)

    row = lax.broadcasted_iota(jnp.int32, (used, LANES), 0)
    total = lax.axis_size("gx") * rows
    base = jnp.maximum(way(shifts) - ITERS, 0)
    start = lax.axis_index("gx") * rows + base
    sets = (work[0:4], work[4:8])
    lane = lax.broadcasted_iota(jnp.int32, (1, LANES), 1)
    half = LANES // 2
    known = {}
    if part == 0:
        known[0] = (0, LANES), (LANES, LANES)
        known[1] = (0, LANES), (half, LANES)
        known[inner - 1] = (0, half), (0, LANES)
        known[inner] = (0, 0), (0, LANES)

    def mask(step):
        offset = shifts[0]
        for earlier in range(step):
            offset = offset + shifts[earlier + 1]
        return row >= offset - start, row < offset + total - start

    def read(step, i, strip):
        if step == 0:
            return source[i][strip, pl.ds(base, used), :]
        return sets[step % 2][i][strip]

    def factor(step, strip):
        if step == 0:
            work_coeff[strip] = source_coeff[strip, pl.ds(base, used), :]
        return work_coeff[strip]

    def write(step, strip, *values):
        later = sets[(step + 1) % 2]
        for ref, value in zip(later, values):
            ref[strip] = value
        if step + 1 < ITERS:
            behind = source_behind[strip, pl.ds(step, 1), :]
            at = pl.ds(rows + ITERS, 1)
            if strip in known:
                lows, highs = known[strip]
                inside = (lane >= jnp.where(low, lows[0], highs[0])) & (lane < jnp.where(low, lows[1], highs[1]))
                behind = jnp.where(inside, behind, values[0][rows + ITERS : rows + ITERS + 1])
            later[0][strip, at, :] = behind
        elif strip in ends:
            group = ends.index(strip)
            first, last = ([0] + ends)[group], strip
            for k in range(first, last):
                lanes = pl.ds(k * LANES, LANES)
                for i, ref in enumerate(later[0:3]):
                    stage[i, :, lanes] = ref[done + k, pl.ds(ITERS, rows), :]
            for i in range(3):
                copies.append(
                    pltpu.make_async_copy(
                        stage.at[i, :, pl.ds(first * LANES, (last - first) * LANES)],
                        outs[i].at[:, pl.ds(pl.multiple_of((column + first) * LANES, LANES), (last - first) * LANES)],
                        sem.at[i, group],
                    )
                )
                copies[-1].start()

    copies = []
    ends = [kept * k // GROUPS for k in range(1, GROUPS + 1)]
    march(ITERS, local, used, read, factor, write, mask)
    for copy in copies:
        copy.wait()


class Plan:
    def __init__(self, rows, cols, moved):
        assert rows % TILE == 0 and cols % LANES == 0
        self.rows = rows
        self.strips = cols // LANES
        self.reach = up(rows + ITERS * SMAX + ITERS, TILE)
        self.used = up(rows + 2 * ITERS, TILE)
        self.head = self.reach - rows
        assert rows >= self.head and self.used <= self.reach
        self.count = (self.strips - OUTER, OUTER)
        self.local = (self.count[0] + 1, OUTER + 2)
        self.moved = moved
        self.place = (0, moved + 1, 2 * moved + 1, 3 * moved + 1)
        self.sent = 3 * moved + ITERS
        first = (self.count[0] - 1) * self.sent
        self.cut = first // TILE * TILE
        self.side = first - self.cut

    def buffer(self, part):
        behind = max(self.place[2] + self.head, self.place[3] + TILE)
        end = (self.count[part] - 1) * self.sent + behind
        return up(max(end, self.count[part] * self.sent + 3 * TILE), TILE)


def call(kernel, name, outs, ins, out_spaces, scratch, aliases=None, flops=1 << 20):
    return pl.pallas_call(
        kernel,
        name=name,
        out_shape=outs,
        in_specs=[spec(space) for space in ins],
        out_specs=[spec(space) for space in out_spaces],
        scratch_shapes=scratch,
        input_output_aliases=aliases or {},
        cost_estimate=pl.CostEstimate(flops=flops, bytes_accessed=flops, transcendentals=0),
        compiler_params=pltpu.CompilerParams(vmem_limit_bytes=16 << 20),
    )


def f32(*shape):
    return VMEM(shape, jnp.float32)


def advance(moved, inner_sent, outer_sent, electric, magnetic_x, magnetic_z, index_map, period_seq, eps_table, shifts):
    rows, cols = electric.shape
    plan = Plan(rows, cols, moved)
    strips, reach = plan.strips, plan.reach
    fields = (electric, magnetic_x, magnetic_z)
    count_x = lax.axis_size("gx")
    back = [(i + 1, i) for i in range(count_x - 1)]
    swap = [(0, 1), (1, 0)]
    leads = [
        lax.ppermute(lax.slice_in_dim(packed, 0, plan.buffer(part), axis=0), "gx", back)
        for part, packed in enumerate((inner_sent, outer_sent))
    ]
    groups = reach // TILE
    edge, *held, coeff = call(
        functools.partial(prepare_kernel, plan),
        "prepare",
        [f32(3 * rows + reach, LANES)] + [f32(strips, reach, LANES)] * 4,
        [pltpu.SMEM] * 2 + [HBM] * 4,
        [VMEM] * 5,
        [
            VMEM((reach, cols), jnp.int32),
            pltpu.SemaphoreType.DMA((3,)),
            pltpu.SemaphoreType.DMA((3, strips)),
            pltpu.SemaphoreType.DMA((groups,)),
        ],
    )(period_seq, eps_table, *fields, index_map)
    halo = lax.ppermute(edge, "gz", swap)
    halo_lead = lax.ppermute(lax.slice_in_dim(leads[0], plan.cut, None, axis=0), "gz", swap)
    outs = ()
    for part in range(2):
        kept = (plan.count[0] - 1, plan.count[1] + 1)[part]
        local = plan.local[part]
        work = [VMEM((local, reach, LANES), jnp.float32)] * 4 + [VMEM((local, TILE, LANES), jnp.float32)]
        work += [VMEM((local, plan.used, LANES), jnp.float32)] * 9
        outs = call(
            functools.partial(update_kernel, plan, part),
            f"update{part}",
            [HBM((rows, cols), jnp.float32)] * 3,
            [pltpu.SMEM] + [VMEM] * (7 + part) + [HBM] * len(outs),
            [HBM] * 3,
            work + [VMEM((3, rows, kept * LANES), jnp.float32), pltpu.SemaphoreType.DMA((3, GROUPS))],
            {8 + part + i: i for i in range(len(outs))},
        )(shifts, *held, coeff, halo, halo_lead, *leads[: 1 + part], *outs)
    return tuple(outs)


def body(electric, magnetic_x, magnetic_z, index_map, period_seq, eps_table, shifts):
    rows, cols = electric.shape
    electric, magnetic_x, magnetic_z, index_map = (
        pltpu.with_memory_space_constraint(item, HBM) for item in (electric, magnetic_x, magnetic_z, index_map)
    )
    tables = [pltpu.with_memory_space_constraint(item, HBM) for item in (period_seq, eps_table, shifts)]
    plan = Plan(rows, cols, BOUNDS[-1])
    strips, head = plan.strips, plan.head
    inner_sent, outer_sent, which, moves = call(
        functools.partial(pack_kernel, plan, BOUNDS),
        "pack",
        [f32(plan.buffer(0), LANES), f32(plan.buffer(1), LANES), pltpu.SMEM((1,), jnp.int32), pltpu.SMEM((ITERS,), jnp.int32)],
        [HBM] * 7,
        [VMEM, VMEM, pltpu.SMEM, pltpu.SMEM],
        [
            pltpu.SMEM(period_seq.shape, jnp.int32),
            pltpu.SMEM(eps_table.shape, jnp.float32),
            pltpu.SMEM(shifts.shape, jnp.int32),
            VMEM((3, head, cols), jnp.float32),
            VMEM((head, cols), jnp.int32),
            VMEM((strips, TILE, LANES), jnp.float32),
        ]
        + [VMEM((strips, TILE, LANES), jnp.float32)] * 3
        + [VMEM((strips, head, LANES), jnp.float32)] * 3
        + [VMEM((strips, head, LANES), jnp.int32)]
        + [VMEM((strips, TILE, LANES), jnp.float32)] * (4 * (ITERS - 1))
        + [pltpu.SemaphoreType.DMA((3 + 4 * head // TILE,))],
    )(*tables, electric, magnetic_x, magnetic_z, index_map)
    rest = (electric, magnetic_x, magnetic_z, index_map, period_seq, eps_table, moves)
    return lax.switch(
        which[0], [functools.partial(advance, bound) for bound in BOUNDS], inner_sent, outer_sent, *rest
    )


def solution(mesh):
    assert mesh.shape["gz"] == 2
    placed = (
        P(("grp", "gx"), "gz"),
        P(("grp", "gx"), "gz"),
        P(("grp", "gx"), "gz"),
        P(None, None, "gz"),
        P("grp"),
        P(),
        P("grp"),
    )
    return jax.shard_map(
        body,
        mesh=mesh,
        in_specs=placed,
        out_specs=(P(("grp", "gx"), "gz"), P(("grp", "gx"), "gz"), P(("grp", "gx"), "gz")),
        check_vma=False,
    )
```

```python
import functools

import jax
import jax.numpy as jnp
from jax import lax
from jax.experimental import pallas as pl
from jax.experimental.pallas import tpu as pltpu
from jax.sharding import PartitionSpec as P

ITERS = 4
SMAX = 4
LANES = 128
TILE = 8
OUTER = 10
AHEAD = 4
GROUPS = 3
BOUNDS = (*range(3 * SMAX - 1, ITERS * SMAX - 1), ITERS * SMAX)

courant = 0.6

VMEM = pltpu.VMEM
HBM = pltpu.HBM


def up(value, unit):
    return -(-value // unit) * unit


def spec(space):
    return pl.BlockSpec(memory_space=space)


def pack_kernel(plan, bounds, moves, e, hx, hz, inner_out, outer_out, which_out, moves_out, shifts, buf, side, sem):
    low = lax.axis_index("gz") == 0
    strips, head = plan.strips, plan.head
    groups = head // TILE
    copies = [
        pltpu.make_async_copy(
            field.at[pl.ds(q * TILE, TILE), :], buf.at[i, pl.ds(q * TILE, TILE), :], sem.at[1 + groups * i + q]
        )
        for i, field in enumerate((e, hx, hz))
        for q in range(groups)
    ]
    copies.append(pltpu.make_async_copy(moves, shifts, sem.at[0]))
    for copy in copies:
        copy.start()
    copies.pop().wait()
    total = way(shifts)
    which = jnp.int32(0)
    bound = jnp.int32(bounds[0])
    for now, after in zip(bounds[:-1], bounds[1:]):
        which = which + (total > now).astype(jnp.int32)
        bound = bound + jnp.where(total > now, after - now, 0)
    for step in range(ITERS):
        moves_out[step] = shifts[step]
    which_out[0] = which
    for copy in copies:
        copy.wait()

    sent = 3 * bound + 1
    place = (0, bound + 1, 2 * bound + 1)
    inner, outer = plan.count

    def put(out, at, strip):
        lanes = pl.ds(pl.multiple_of(strip * LANES, LANES), LANES)
        for i in range(3):
            for q in range(groups):
                out[pl.ds(at + place[i] + q * TILE, TILE), :] = buf[i, pl.ds(q * TILE, TILE), lanes]

    for k in range(inner):
        put(inner_out, k * sent, jnp.where(low, outer + k, inner - 1 - k))
    lanes = pl.ds(pl.multiple_of(jnp.where(low, strips - 1, 0) * LANES, LANES), LANES)
    for i in range(3):
        side[i] = buf[i, :, lanes]
        inner_out[pl.ds(inner * sent + i * TILE, TILE), :] = side[i, pl.ds(bound, TILE), :]
    for k in range(outer):
        put(outer_out, k * sent, jnp.where(low, k, inner + k))


def behind_kernel(plan, period_seq, eps, shifts, e, hx, hz, index_map, out, buf, levels, coeff, *scratch):
    fields, source, source_levels, work, sem = scratch[0:3], scratch[3:6], scratch[6], scratch[7:-1], scratch[-1]
    strips, head = plan.strips, plan.head
    groups = head // TILE
    copies = [
        pltpu.make_async_copy(field.at[pl.ds(0, head), :], buf.at[i], sem.at[i]) for i, field in enumerate((e, hx, hz))
    ]
    for group in range(groups):
        copies.append(
            pltpu.make_async_copy(
                map_rows(plan, period_seq, index_map, group, 0, strips * LANES),
                levels.at[pl.ds(group * TILE, TILE), :],
                sem.at[3 + group],
            )
        )
    for copy in copies:
        copy.start()
    base = jnp.maximum(way(shifts) - ITERS, 0)
    inverse = inverse_table(eps)
    for copy in copies:
        copy.wait()
    for strip in range(strips):
        lanes = pl.ds(strip * LANES, LANES)
        for i in range(3):
            source[i][strip] = buf[i, :, lanes]
        source_levels[strip] = levels[:, lanes]
    sets = [fields] + [work[4 * k : 4 * k + 4] for k in range(ITERS - 1)]

    def read(step, i, strip):
        if step == 0:
            return source[i][strip, pl.ds(base, TILE), :]
        return sets[step][i][strip]

    def factor(step, strip):
        if step == 0:
            coeff[strip] = material_of(source_levels[strip, pl.ds(base, TILE), :], inverse)
        return coeff[strip]

    def write(step, strip, *values):
        for ref, value in zip(sets[step + 1], values):
            ref[strip] = value
        out[pl.ds(strip * (ITERS - 1) + step, 1), :] = values[0][ITERS : ITERS + 1]

    march(ITERS - 1, strips, TILE, read, factor, write)


def way(shifts):
    total = shifts[0]
    for step in range(1, ITERS):
        total = total + shifts[step]
    return total


def march(steps, strips, used, read, factor, write, mask=None):
    lane = lax.broadcasted_iota(jnp.int32, (used, LANES), 1)
    last_lane, first_lane = lane == LANES - 1, lane == 0
    none = jnp.zeros((used, LANES), jnp.float32)
    for step in range(steps):
        above, below = mask(step) if mask else (None, None)
        values, left, right, hx_right = {}, {strips: none}, {-1: none}, {-1: none}
        for strip in range(-AHEAD, strips):
            coming = strip + AHEAD
            if coming < strips:
                values[coming] = read(step, 0, coming)
                left[coming] = pltpu.roll(values[coming], LANES - 1, 1)
                right[coming] = pltpu.roll(values[coming], 1, 1)
                if step == 0:
                    hx_right[coming] = pltpu.roll(read(step, 1, coming), 1, 1)
            if strip < 0:
                continue
            field_e = values.pop(strip)
            upper = jnp.where(last_lane, left[strip + 1], left[strip])
            under = jnp.where(first_lane, right[strip - 1], right[strip])
            if step == 0:
                lower = jnp.where(first_lane, hx_right[strip - 1], hx_right[strip])
            else:
                lower = read(step, 3, strip)
            field_hx = read(step, 1, strip) + courant * (upper - field_e)
            lower = lower + courant * (field_e - under)
            if strip == 0:
                lower = jnp.where(first_lane, 0.0, lower)
            ahead = pltpu.roll(field_e, used - 1, 0)
            field_hz = read(step, 2, strip) - courant * (ahead - field_e)
            if above is not None:
                field_hz = jnp.where(above, field_hz, 0.0)
            behind = pltpu.roll(field_hz, 1, 0)
            moved = field_e + factor(step, strip) * ((field_hx - lower) - (field_hz - behind))
            if below is not None:
                moved = jnp.where(below, moved, 0.0)
            write(step, strip, moved, field_hx, field_hz, lower)


def material_of(levels, inverse):
    result = jnp.zeros(levels.shape, jnp.float32)
    for level, value in enumerate(inverse):
        result = jnp.where(levels == level, value, result)
    return result


def inverse_table(eps):
    return [courant * (1.0 / jnp.full((TILE, LANES), eps[i], jnp.float32)) for i in range(eps.shape[0])]


def map_rows(plan, period_seq, index_map, group, first, width):
    span = index_map.shape[1]
    cell = lax.axis_index("gx") * plan.rows + group * TILE
    period = jnp.minimum(cell // span, period_seq.shape[0] - 1)
    phase = pl.multiple_of(cell % span, TILE)
    return index_map.at[period_seq[period], pl.ds(phase, TILE), pl.ds(first, width)]


def prepare_kernel(
    plan, period_seq, eps, e, hx, hz, index_map, edge, e_out, hx_out, hz_out, coeff,
    levels, edge_sem, field_sem, sem,
):
    low = lax.axis_index("gz") == 0
    first = pl.multiple_of(jnp.where(low, plan.strips - 1, 0) * LANES, LANES)
    rows, strips = plan.rows, plan.strips
    groups = plan.reach // TILE
    fields = (e, hx, hz)
    edges = [
        pltpu.make_async_copy(
            field.at[:, pl.ds(first, LANES)], edge.at[pl.ds(i * rows, rows), :], edge_sem.at[i]
        )
        for i, field in enumerate(fields)
    ]
    maps = [
        pltpu.make_async_copy(
            map_rows(plan, period_seq, index_map, group, 0, strips * LANES),
            levels.at[pl.ds(group * TILE, TILE), :],
            sem.at[group],
        )
        for group in range(groups)
    ]
    for copy in edges + maps:
        copy.start()

    def field_copy(i, strip):
        return pltpu.make_async_copy(
            fields[i].at[:, pl.ds(pl.multiple_of(strip * LANES, LANES), LANES)],
            (e_out, hx_out, hz_out)[i].at[strip, pl.ds(0, rows), :],
            field_sem.at[i, strip],
        )

    def start_strip(strip, _):
        for i in range(3):
            field_copy(i, strip).start()
        return 0

    lax.fori_loop(0, strips, start_strip, 0)
    inverse = inverse_table(eps)
    for copy in maps:
        copy.wait()

    def strip_of(strip, _):
        lanes = pl.ds(pl.multiple_of(strip * LANES, LANES), LANES)
        for group in range(groups):
            at = pl.ds(group * TILE, TILE)
            coeff[strip, at, :] = material_of(levels[at, lanes], inverse)
        return 0

    lax.fori_loop(0, strips, strip_of, 0, unroll=2)
    for group in range(groups):
        at = pl.ds(group * TILE, TILE)
        edge[pl.ds(3 * rows + group * TILE, TILE), :] = material_of(levels[at, pl.ds(first, LANES)], inverse)
    for copy in edges:
        copy.wait()

    def wait_strip(strip, _):
        for i in range(3):
            field_copy(i, strip).wait()
        return 0

    lax.fori_loop(0, strips, wait_strip, 0)


def update_kernel(plan, part, shifts, *refs):
    fields, coeff, halo, halo_lead, behinds, leads = refs[0:3], refs[3], refs[4], refs[5], refs[6], refs[7 : 8 + part]
    refs = refs[8 + part :]
    if part:
        refs = refs[3:]
    outs, source, source_coeff, source_behind = refs[0:3], refs[3:6], refs[6], refs[7]
    work, work_coeff, stage, sem = refs[8:16], refs[16], refs[17], refs[18]
    low = lax.axis_index("gz") == 0
    rows, reach, used = plan.rows, plan.reach, plan.used
    lead_rows = reach - rows
    local = plan.local[part]

    def own(strip, to):
        for i in range(3):
            source[i][to, pl.ds(0, rows), :] = fields[i][strip, pl.ds(0, rows), :]
        source_coeff[to] = coeff[strip]
        source_behind[to] = behinds[pl.ds(strip * (ITERS - 1), TILE), :]

    def lead(sent, at, to):
        for i in range(3):
            for q in range(lead_rows // TILE):
                source[i][to, pl.ds(rows + q * TILE, TILE), :] = sent[pl.ds(at + plan.place[i] + q * TILE, TILE), :]

    def lead_side(sent, at, to):
        for i in range(3):
            source[i][to, pl.ds(rows + plan.moved, TILE), :] = sent[pl.ds(at + i * TILE, TILE), :]

    inner, outer = plan.count
    if part == 0:
        for k in range(inner):
            strip = jnp.where(low, outer + k, inner - 1 - k)
            to = jnp.where(low, k, inner - k)
            own(strip, to)
            lead(leads[0], k * plan.sent, to)
        lead_side(leads[0], inner * plan.sent, jnp.where(low, inner - 1, 1))
        side = jnp.where(low, inner, 0)
        for i in range(3):
            source[i][side, pl.ds(0, rows), :] = halo[pl.ds(i * rows, rows), :]
        source_coeff[side] = halo[pl.ds(3 * rows, reach), :]
        source_behind[side] = jnp.zeros((TILE, LANES), jnp.float32)
        lead(halo_lead, plan.side, side)
        lead_side(halo_lead, plan.side + plan.sent, side)
        done, kept = 1, inner - 1
        column = jnp.where(low, outer + 1, 0)
    else:
        for k in range(outer):
            to = jnp.where(low, k, k + 2)
            own(jnp.where(low, k, inner + k), to)
            lead(leads[1], k * plan.sent, to)
        for k in range(2):
            to = jnp.where(low, outer + k, 1 - k)
            own(jnp.where(low, outer + k, inner - 1 - k), to)
            lead(leads[0], k * plan.sent, to)
        done, kept = jnp.where(low, 0, 1), outer + 1
        column = jnp.where(low, 0, inner - 1)

    row = lax.broadcasted_iota(jnp.int32, (used, LANES), 0)
    total = lax.axis_size("gx") * rows
    base = jnp.maximum(way(shifts) - ITERS, 0)
    start = lax.axis_index("gx") * rows + base
    sets = (work[0:4], work[4:8])
    lane = lax.broadcasted_iota(jnp.int32, (1, LANES), 1)
    half = LANES // 2
    known = {}
    if part == 0:
        known[0] = (0, LANES), (LANES, LANES)
        known[1] = (0, LANES), (half, LANES)
        known[inner - 1] = (0, half), (0, LANES)
        known[inner] = (0, 0), (0, LANES)

    def mask(step):
        offset = shifts[0]
        for earlier in range(step):
            offset = offset + shifts[earlier + 1]
        return row >= offset - start, row < offset + total - start

    def read(step, i, strip):
        if step == 0:
            return source[i][strip, pl.ds(base, used), :]
        return sets[step % 2][i][strip]

    def factor(step, strip):
        if step == 0:
            work_coeff[strip] = source_coeff[strip, pl.ds(base, used), :]
        return work_coeff[strip]

    def write(step, strip, *values):
        later = sets[(step + 1) % 2]
        for ref, value in zip(later, values):
            ref[strip] = value
        if step + 1 < ITERS:
            behind = source_behind[strip, pl.ds(step, 1), :]
            at = pl.ds(rows + ITERS, 1)
            if strip in known:
                lows, highs = known[strip]
                inside = (lane >= jnp.where(low, lows[0], highs[0])) & (lane < jnp.where(low, lows[1], highs[1]))
                behind = jnp.where(inside, behind, values[0][rows + ITERS : rows + ITERS + 1])
            later[0][strip, at, :] = behind
        elif strip in ends:
            group = ends.index(strip)
            first, last = ([0] + ends)[group], strip
            for k in range(first, last):
                lanes = pl.ds(k * LANES, LANES)
                for i, ref in enumerate(later[0:3]):
                    stage[i, :, lanes] = ref[done + k, pl.ds(ITERS, rows), :]
            for i in range(3):
                copies.append(
                    pltpu.make_async_copy(
                        stage.at[i, :, pl.ds(first * LANES, (last - first) * LANES)],
                        outs[i].at[:, pl.ds(pl.multiple_of((column + first) * LANES, LANES), (last - first) * LANES)],
                        sem.at[i, group],
                    )
                )
                copies[-1].start()

    copies = []
    ends = [kept * k // GROUPS for k in range(1, GROUPS + 1)]
    march(ITERS, local, used, read, factor, write, mask)
    for copy in copies:
        copy.wait()


class Plan:
    def __init__(self, rows, cols, moved):
        assert rows % TILE == 0 and cols % LANES == 0
        self.rows = rows
        self.strips = cols // LANES
        self.reach = up(rows + ITERS * SMAX + ITERS, TILE)
        self.used = up(rows + 2 * ITERS, TILE)
        self.head = self.reach - rows
        assert rows >= self.head and self.used <= self.reach
        self.count = (self.strips - OUTER, OUTER)
        self.local = (self.count[0] + 1, OUTER + 2)
        self.moved = moved
        self.place = (0, moved + 1, 2 * moved + 1)
        self.sent = 3 * moved + 1
        self.behind = up((self.strips - 1) * (ITERS - 1) + TILE, TILE)
        first = (self.count[0] - 1) * self.sent
        self.cut = first // TILE * TILE
        self.side = first - self.cut

    def buffer(self, part):
        end = (self.count[part] - 1) * self.sent + self.place[2] + self.head
        return up(max(end, self.count[part] * self.sent + 3 * TILE), TILE)


def call(kernel, outs, ins, out_spaces, scratch, aliases=None, flops=1 << 20):
    return pl.pallas_call(
        kernel,
        out_shape=outs,
        in_specs=[spec(space) for space in ins],
        out_specs=[spec(space) for space in out_spaces],
        scratch_shapes=scratch,
        input_output_aliases=aliases or {},
        cost_estimate=pl.CostEstimate(flops=flops, bytes_accessed=flops, transcendentals=0),
        compiler_params=pltpu.CompilerParams(vmem_limit_bytes=16 << 20),
    )


def f32(*shape):
    return VMEM(shape, jnp.float32)


def branch(moved, *args):
    return advance(moved, *args)


def advance(moved, inner_sent, outer_sent, electric, magnetic_x, magnetic_z, index_map, period_seq, eps_table, shifts):
    rows, cols = electric.shape
    plan = Plan(rows, cols, moved)
    strips, reach = plan.strips, plan.reach
    fields = (electric, magnetic_x, magnetic_z)
    count_x = lax.axis_size("gx")
    back = [(i + 1, i) for i in range(count_x - 1)]
    swap = [(0, 1), (1, 0)]
    head = plan.head
    inner_lead, outer_lead = (
        lax.slice_in_dim(packed, 0, plan.buffer(part), axis=0) for part, packed in enumerate((inner_sent, outer_sent))
    )
    inner_lead = lax.ppermute(inner_lead, "gx", back)
    behind = call(
        functools.partial(behind_kernel, plan),
        [f32(plan.behind, LANES)],
        [pltpu.SMEM] * 3 + [HBM] * 4,
        [VMEM],
        [
            VMEM((3, head, cols), jnp.float32),
            VMEM((head, cols), jnp.int32),
            VMEM((strips, TILE, LANES), jnp.float32),
        ]
        + [VMEM((strips, TILE, LANES), jnp.float32)] * 3
        + [VMEM((strips, head, LANES), jnp.float32)] * 3
        + [VMEM((strips, head, LANES), jnp.int32)]
        + [VMEM((strips, TILE, LANES), jnp.float32)] * (4 * (ITERS - 1))
        + [pltpu.SemaphoreType.DMA((3 + head // TILE,))],
    )(period_seq, eps_table, shifts, *fields, index_map)[0]
    behind = lax.ppermute(behind, "gx", back)
    outer_lead = lax.ppermute(outer_lead, "gx", back)
    leads = (inner_lead, outer_lead)
    groups = reach // TILE
    edge, *held, coeff = call(
        functools.partial(prepare_kernel, plan),
        [f32(3 * rows + reach, LANES)] + [f32(strips, reach, LANES)] * 4,
        [pltpu.SMEM] * 2 + [HBM] * 4,
        [VMEM] * 5,
        [
            VMEM((reach, cols), jnp.int32),
            pltpu.SemaphoreType.DMA((3,)),
            pltpu.SemaphoreType.DMA((3, strips)),
            pltpu.SemaphoreType.DMA((groups,)),
        ],
    )(period_seq, eps_table, *fields, index_map)
    halo = lax.ppermute(edge, "gz", swap)
    halo_lead = lax.ppermute(lax.slice_in_dim(leads[0], plan.cut, None, axis=0), "gz", swap)
    outs = ()
    for part in range(2):
        kept = (plan.count[0] - 1, plan.count[1] + 1)[part]
        local = plan.local[part]
        work = [VMEM((local, reach, LANES), jnp.float32)] * 4 + [VMEM((local, TILE, LANES), jnp.float32)]
        work += [VMEM((local, plan.used, LANES), jnp.float32)] * 9
        outs = call(
            functools.partial(update_kernel, plan, part),
            [HBM((rows, cols), jnp.float32)] * 3,
            [pltpu.SMEM] + [VMEM] * (8 + part) + [HBM] * len(outs),
            [HBM] * 3,
            work + [VMEM((3, rows, kept * LANES), jnp.float32), pltpu.SemaphoreType.DMA((3, GROUPS))],
            {9 + part + i: i for i in range(len(outs))},
        )(shifts, *held, coeff, halo, halo_lead, behind, *leads[: 1 + part], *outs)
    return tuple(outs)


def body(electric, magnetic_x, magnetic_z, index_map, period_seq, eps_table, shifts):
    rows, cols = electric.shape
    electric, magnetic_x, magnetic_z, index_map = (
        pltpu.with_memory_space_constraint(item, HBM) for item in (electric, magnetic_x, magnetic_z, index_map)
    )
    moves = pltpu.with_memory_space_constraint(shifts, HBM)
    plan = Plan(rows, cols, BOUNDS[-1])
    head = plan.head
    inner_sent, outer_sent, which, moves = call(
        functools.partial(pack_kernel, plan, BOUNDS),
        [f32(plan.buffer(0), LANES), f32(plan.buffer(1), LANES), pltpu.SMEM((1,), jnp.int32), pltpu.SMEM((ITERS,), jnp.int32)],
        [HBM] * 4,
        [VMEM, VMEM, pltpu.SMEM, pltpu.SMEM],
        [
            pltpu.SMEM(shifts.shape, jnp.int32),
            VMEM((3, head, cols), jnp.float32),
            VMEM((3, head, LANES), jnp.float32),
            pltpu.SemaphoreType.DMA((1 + 3 * head // TILE,)),
        ],
    )(moves, electric, magnetic_x, magnetic_z)
    rest = (electric, magnetic_x, magnetic_z, index_map, period_seq, eps_table, moves)
    return lax.switch(
        which[0], [functools.partial(branch, bound) for bound in BOUNDS], inner_sent, outer_sent, *rest
    )


def solution(mesh):
    assert mesh.shape["gz"] == 2
    placed = (
        P(("grp", "gx"), "gz"),
        P(("grp", "gx"), "gz"),
        P(("grp", "gx"), "gz"),
        P(None, None, "gz"),
        P("grp"),
        P(),
        P("grp"),
    )
    return jax.shard_map(
        body,
        mesh=mesh,
        in_specs=placed,
        out_specs=(P(("grp", "gx"), "gz"), P(("grp", "gx"), "gz"), P(("grp", "gx"), "gz")),
        check_vma=False,
    )
```
